32 devices in a mesh: groups: 2 (over x), ctx: 16 (over z, y, core).
Axes of the slice: x: 2, y: 2, z: 4, core: 2. Of those that a mesh axis runs over, the one named last changes fastest.
Arguments:
- queries: bfloat16 [8192, 1024], P(('groups', 'ctx')), parts along dimension 0, may hold values from -7 to 7
- keys: bfloat16 [8192, 128], P(('groups', 'ctx')), parts along dimension 0, may hold values from -7 to 7
- values: bfloat16 [8192, 128], P(('groups', 'ctx')), parts along dimension 0, may hold values from -6 to 6
- span_order: int32 [64], P('groups'), parts along dimension 0, may hold values from 0 to 31, as said below
Outputs:
- attended: bfloat16 [8192, 1024], P(('groups', 'ctx')), parts along dimension 0
The draws below stay inside these ranges and needn't reach their ends.
There are 2 independent parts, one for each index of `groups`. The reference program is written for one: setup_inputs(seed, part) draws one part's arguments, and reference() takes and returns one part's arrays. A program takes and returns all parts, laid end to end along the dimension named above; each array names one. Nothing has to cross between parts.
Inputs may be any that keep to these rules, and one draw needn't show every extreme that they name: A permutation: rows j * 128 to (j + 1) * 128 - 1 hold span span_order[j] of the sequence; for every j, span_order[2 j] + span_order[2 j + 1] = 31.
All inputs are finite; a program needn't handle non-finite values.
Results may differ from the reference program's by a relative error of at most 0.006.
Values may be sent and summed in bfloat16 or wider, within the bound.
A program may use at most 64 MiB of HBM per device.

```python
import math
import jax
import jax.numpy as jnp
from jax import lax

QH = 8
DH = 128
SPAN = 128
SEQ = 4096
NSPAN = 32


def drawn_pair(key):
    query_key = jax.random.fold_in(key, 11)
    keys_key = jax.random.fold_in(key, 12)
    query_draw = jnp.clip(jax.random.normal(query_key, (SEQ, QH * DH), jnp.float32), -5.0, 5.0)
    keys_draw = jnp.clip(jax.random.normal(keys_key, (SEQ, DH), jnp.float32), -5.0, 5.0)
    return (query_draw, keys_draw)


def draw_queries(key, part):
    return drawn_pair(key)[0].astype(jnp.bfloat16)


def draw_keys(key, part):
    return drawn_pair(key)[1].astype(jnp.bfloat16)


def draw_span_order(key, part):
    half = NSPAN // 2
    pairs = jax.random.permutation(jax.random.fold_in(key, 21), half).astype(jnp.int32)
    flipped = jax.random.randint(jax.random.fold_in(key, 22), (half,), 0, 2)
    early = pairs
    late = (NSPAN - 1 - pairs).astype(jnp.int32)
    first = jnp.where(flipped == 1, late, early)
    second = jnp.where(flipped == 1, early, late)
    return jnp.stack([first, second], axis=1).reshape(NSPAN).astype(jnp.int32)


def shard_levels(stream_key, shape, cuts, smallest, top_value):
    factor_of = 1.0
    for dim, parts in cuts:
        draws = jax.random.uniform(jax.random.fold_in(jax.random.fold_in(stream_key, 6), dim), (parts,), jnp.float32, smallest / len(cuts), top_value / len(cuts))
        factor_of = factor_of * jnp.repeat(jnp.exp(draws), shape[dim] // parts).reshape((-1,) + (1,) * (len(shape) - 1 - dim))
    return factor_of


def noise(stream_key, shape, width, most, cuts=(), held_as=jnp.bfloat16):
    array = width * jax.random.normal(stream_key, shape, jnp.float32)
    if cuts:
        array = array * shard_levels(stream_key, shape, cuts, -0.22, 0.18)
    return jnp.clip(array, -most, most).astype(held_as)


def setup_inputs(seed: int = 0, part: int = 0) -> dict:
    arg_keys = jax.random.split(jax.random.key(seed), 5)
    own_keys = jax.random.split(jax.random.fold_in(arg_keys[4], part), 5)
    return {
        "queries": draw_queries(jax.random.fold_in(jax.random.fold_in(arg_keys[4], part), 71), part),
        "keys": draw_keys(jax.random.fold_in(jax.random.fold_in(arg_keys[4], part), 71), part),
        "values": noise(own_keys[2], (SEQ, DH), 1.0, 6.0, ((0, 16),)),
        "span_order": draw_span_order(jax.random.fold_in(jax.random.fold_in(arg_keys[4], part), 71), part),
    }


def reference(queries, keys, values, span_order):
    total_rows = queries.shape[0]
    rows = jnp.arange(total_rows, dtype=jnp.int32)
    position = (span_order[rows // SPAN] * SPAN + rows % SPAN).astype(jnp.int32)
    block = math.gcd(total_rows, 512)
    scale = 1.0 / math.sqrt(DH)
    keys_f = keys.astype(jnp.float32)
    values_f = values.astype(jnp.float32)

    def one_block(index):
        first = (index * block).astype(jnp.int32)
        query_blk = lax.dynamic_slice_in_dim(queries, first, block, 0).reshape(block, QH, DH).astype(jnp.float32)
        query_pos = lax.dynamic_slice_in_dim(position, first, block, 0)
        score = jnp.einsum('qhd,kd->hqk', query_blk, keys_f) * scale
        kept = position[None, None, :] <= query_pos[None, :, None]
        score = jnp.where(kept, score, jnp.float32(-1e+30))
        top = lax.optimization_barrier(jnp.max(score, axis=-1, keepdims=True))
        weight = jnp.where(kept, jnp.exp(score - top), jnp.float32(0.0))
        total = lax.optimization_barrier(jnp.sum(weight, axis=-1))
        weight_b = lax.optimization_barrier(weight.astype(jnp.bfloat16)).astype(jnp.float32)
        mixed = jnp.einsum('hqk,kd->hqd', weight_b, values_f) / total[:, :, None]
        return jnp.transpose(mixed, (1, 0, 2)).reshape(block, QH * DH).astype(jnp.bfloat16)
    outputs = lax.map(one_block, jnp.arange(total_rows // block, dtype=jnp.int32))
    return outputs.reshape(total_rows, QH * DH)
```

```python
import functools
import math

import jax
import jax.numpy as jnp
from jax import lax
from jax.experimental import pallas as pl
from jax.experimental.pallas import tpu as pltpu
from jax.sharding import PartitionSpec as P

UP, DOWN, SIDE, TWIN = 0, 1, 2, 3
NEG = -1e30


def gather_kernel(n, k_ref, v_ref, buf, send_sem, recv_sem):
    lanes = 4
    zs = n // lanes
    me = lax.axis_index("ctx")
    z = me // lanes
    lane = lax.rem(me, lanes)
    y = lane // 2
    c = lax.rem(lane, 2)
    side = z * lanes + (1 - y) * 2 + c
    twin = z * lanes + y * 2 + (1 - c)
    not_top = z < zs - 1
    not_bottom = z > 0
    up = jnp.minimum(me + lanes, n - lanes + lane)
    down = jnp.maximum(me - lanes, lane)
    target = (up, down, side, twin)

    barrier = pltpu.get_barrier_semaphore()

    def greet(who):
        pl.semaphore_signal(
            barrier, inc=1, device_id={"ctx": who}, device_id_type=pl.DeviceIdType.MESH
        )

    greet(side)
    greet(twin)
    pl.when(not_top)(lambda: greet(up))
    pl.when(not_bottom)(lambda: greet(down))
    pl.semaphore_wait(barrier, 2 + not_top.astype(jnp.int32) + not_bottom.astype(jnp.int32))

    def copy(block, kv, route, src=None):
        return pltpu.make_async_remote_copy(
            src_ref=buf.at[block, kv] if src is None else src,
            dst_ref=buf.at[block, kv],
            send_sem=send_sem.at[block, kv, route],
            recv_sem=recv_sem.at[block, kv],
            device_id={"ctx": target[route]},
            device_id_type=pl.DeviceIdType.MESH,
        )

    own = (k_ref, v_ref)
    for kv in range(2):
        pl.when(not_top)(lambda: copy(me, kv, UP, own[kv]).start())
        pl.when(not_bottom)(lambda: copy(me, kv, DOWN, own[kv]).start())
        copy(me, kv, SIDE, own[kv]).start()
        copy(me, kv, TWIN, own[kv]).start()
    buf[me, 0] = k_ref[...]
    buf[me, 1] = v_ref[...]

    def at(zz, yy, cc):
        return zz * lanes + yy * 2 + cc

    def from_line(zz, onward, keep):
        block = at(zz, y, c)
        for kv in range(2):
            copy(block, kv, onward).wait_recv()
            pl.when(keep)(lambda: copy(block, kv, onward).start())
            copy(block, kv, SIDE).start()
            copy(block, kv, TWIN).start()

    def from_side(zz):
        block = at(zz, 1 - y, c)
        for kv in range(2):
            copy(block, kv, TWIN).wait_recv()
            copy(block, kv, TWIN).start()

    def from_twin(zz):
        for yy in (y, 1 - y):
            for kv in range(2):
                copy(at(zz, yy, 1 - c), kv, TWIN).wait_recv()

    def both(s, low, high):
        pl.when(z >= s)(lambda: low(z - s))
        pl.when(z + s < zs)(lambda: high(z + s))

    for s in range(1, zs):
        both(s, lambda zz: from_line(zz, UP, not_top), lambda zz: from_line(zz, DOWN, not_bottom))
        if s == 1:
            from_side(z)
        else:
            both(s - 1, from_side, from_side)
    both(zs - 1, from_side, from_side)
    from_twin(z)
    for s in range(1, zs):
        both(s, from_twin, from_twin)

    for kv in range(2):
        pl.when(not_top)(lambda: copy(me, kv, UP, own[kv]).wait_send())
        pl.when(not_bottom)(lambda: copy(me, kv, DOWN, own[kv]).wait_send())
        copy(me, kv, SIDE, own[kv]).wait_send()
        copy(me, kv, TWIN, own[kv]).wait_send()

    def line_sent(zz, onward, keep):
        for kv in range(2):
            pl.when(keep)(lambda: copy(at(zz, y, c), kv, onward).wait_send())
            copy(at(zz, y, c), kv, SIDE).wait_send()
            copy(at(zz, y, c), kv, TWIN).wait_send()

    def side_sent(zz):
        for kv in range(2):
            copy(at(zz, 1 - y, c), kv, TWIN).wait_send()

    side_sent(z)
    for s in range(1, zs):
        both(s, lambda zz: line_sent(zz, UP, not_top), lambda zz: line_sent(zz, DOWN, not_bottom))
        both(s, side_sent, side_sent)


def attend_kernel(n, heads, span, q_ref, kv_ref, order_ref, out_ref, kl, vl, lim, top, acc):
    head_size = kl.shape[1]
    me = lax.axis_index("ctx")
    first = order_ref[2 * me]
    second = order_ref[2 * me + 1]
    p = jnp.minimum(first, second)
    low_at = (second < first).astype(jnp.int32)
    chunks_low = (p + 2) // 2
    base = 2 * chunks_low
    slots = 2 * (n + 1)

    def put(slot, block, half, limit):
        dst = pl.ds(pl.multiple_of(slot * span, span), span)
        src = pl.ds(pl.multiple_of(half * span, span), span)
        kl[dst, :] = kv_ref[block, 0, src, :]
        vl[dst, :] = kv_ref[block, 1, src, :]
        lim[slot] = limit

    put(base - 1, me, low_at, -span)
    put(slots - 1, me, low_at, -span)
    put(0, me, low_at, 0)
    put(base, me, 1 - low_at, 0)

    def place(d, carry):
        q = jnp.minimum(order_ref[2 * d], order_ref[2 * d + 1])
        lo = (order_ref[2 * d + 1] < order_ref[2 * d]).astype(jnp.int32)

        @pl.when(q < p)
        def _():
            put(q + 1, d, lo, span)

        @pl.when(q > p)
        def _():
            put(base + q - p, d, 1 - lo, span)

        put(base + n - p + d, d, lo, span)
        return carry

    lax.fori_loop(0, n, place, 0)

    top[...] = jnp.full_like(top, NEG)
    acc[...] = jnp.zeros_like(acc)
    factor = math.log2(math.e) / math.sqrt(head_size)
    ones = jnp.ones((2 * span, head_size), jnp.bfloat16)
    ahead = lax.broadcasted_iota(jnp.int32, (span, span), 1) - lax.broadcasted_iota(
        jnp.int32, (span, span), 0
    )

    def step(i, carry):
        high = (i >= chunks_low).astype(jnp.int32)
        half = jnp.where(high == 1, 1 - low_at, low_at)
        rows = pl.ds(pl.multiple_of(half * span, span), span)
        at = pl.ds(pl.multiple_of(i * 2 * span, 2 * span), 2 * span)
        keys = kl[at, :]
        vals = jnp.concatenate([vl[at, :], ones], axis=1)
        kept = jnp.concatenate([ahead <= lim[2 * i], ahead <= lim[2 * i + 1]], axis=1)
        for h in range(heads):
            q = q_ref[rows, h * head_size : (h + 1) * head_size]
            score = lax.dot_general(
                q, keys, (((1,), (1,)), ((), ())), preferred_element_type=jnp.float32
            )
            score = jnp.where(kept, score * factor, NEG)
            old = top[high, h]
            fresh = jnp.maximum(old, jnp.max(score, axis=1, keepdims=True))
            weight = jnp.exp2(score - jnp.concatenate([fresh, fresh], axis=1))
            fade = jnp.exp2(old - fresh)
            add = jnp.dot(
                weight.astype(jnp.bfloat16), vals, preferred_element_type=jnp.float32
            )
            acc[high, h] = acc[high, h] * jnp.concatenate([fade, fade], axis=1) + add
            top[high, h] = fresh
        return carry

    lax.fori_loop(0, n + 1, step, 0)

    for t in range(2):
        half = jnp.where(t == 1, 1 - low_at, low_at)
        rows = pl.ds(pl.multiple_of(half * span, span), span)
        for h in range(heads):
            out_ref[rows, h * head_size : (h + 1) * head_size] = (
                acc[t, h, :, :head_size] / acc[t, h, :, head_size:]
            ).astype(jnp.bfloat16)


def body(n, queries, keys, values, span_order):
    local_rows, width = queries.shape
    head_size = keys.shape[1]
    heads = width // head_size
    span = local_rows // 2
    vmem = pl.BlockSpec(memory_space=pltpu.VMEM)
    gathered = pl.pallas_call(
        functools.partial(gather_kernel, n),
        out_shape=jax.ShapeDtypeStruct((n, 2, local_rows, head_size), jnp.bfloat16),
        in_specs=[vmem, vmem],
        out_specs=vmem,
        scratch_shapes=[
            pltpu.SemaphoreType.DMA((n, 2, 4)),
            pltpu.SemaphoreType.DMA((n, 2)),
        ],
        compiler_params=pltpu.CompilerParams(collective_id=0, has_side_effects=True),
        name="gather",
    )(keys, values)
    slots = 2 * (n + 1)
    return pl.pallas_call(
        functools.partial(attend_kernel, n, heads, span),
        out_shape=jax.ShapeDtypeStruct((local_rows, width), jnp.bfloat16),
        in_specs=[vmem, vmem, pl.BlockSpec(memory_space=pltpu.SMEM)],
        out_specs=vmem,
        scratch_shapes=[
            pltpu.VMEM((slots * span, head_size), jnp.bfloat16),
            pltpu.VMEM((slots * span, head_size), jnp.bfloat16),
            pltpu.SMEM((slots,), jnp.int32),
            pltpu.VMEM((2, heads, span, head_size), jnp.float32),
            pltpu.VMEM((2, heads, span, 2 * head_size), jnp.float32),
        ],
        name="attend",
    )(queries, gathered, span_order)


def solution(mesh):
    in_specs = (
        P(("groups", "ctx"), None),
        P(("groups", "ctx"), None),
        P(("groups", "ctx"), None),
        P("groups"),
    )
    out_specs = P(("groups", "ctx"), None)
    return jax.shard_map(
        functools.partial(body, mesh.shape["ctx"]),
        mesh=mesh,
        in_specs=in_specs,
        out_specs=out_specs,
        check_vma=False,
    )
```

```python
import functools
import math

import jax
import jax.numpy as jnp
from jax import lax
from jax.experimental import pallas as pl
from jax.experimental.pallas import tpu as pltpu
from jax.sharding import PartitionSpec as P

UP, DOWN, SIDE, TWIN = 0, 1, 2, 3
NEG = -1e30


def attend_kernel(
    n,
    heads,
    span,
    q_ref,
    k_ref,
    v_ref,
    order_ref,
    out_ref,
    buf,
    qs,
    k1,
    v1,
    k2,
    v2,
    top,
    part,
    acc,
    mix,
    send_sem,
    recv_sem,
):
    head_size = k1.shape[1]
    lanes = 4
    zs = n // lanes
    me = lax.axis_index("ctx")
    z = me // lanes
    lane = lax.rem(me, lanes)
    y = lane // 2
    c = lax.rem(lane, 2)
    side = z * lanes + (1 - y) * 2 + c
    twin = z * lanes + y * 2 + (1 - c)
    not_top = z < zs - 1
    not_bottom = z > 0
    up = jnp.minimum(me + lanes, n - lanes + lane)
    down = jnp.maximum(me - lanes, lane)

    barrier = pltpu.get_barrier_semaphore()

    def greet(who):
        pl.semaphore_signal(
            barrier, inc=1, device_id={"ctx": who}, device_id_type=pl.DeviceIdType.MESH
        )

    greet(side)
    greet(twin)
    pl.when(not_top)(lambda: greet(up))
    pl.when(not_bottom)(lambda: greet(down))
    pl.semaphore_wait(barrier, 2 + not_top.astype(jnp.int32) + not_bottom.astype(jnp.int32))

    def copy(block, kv, route, to, src=None):
        return pltpu.make_async_remote_copy(
            src_ref=buf.at[block, kv] if src is None else src,
            dst_ref=buf.at[block, kv],
            send_sem=send_sem.at[block, kv, route],
            recv_sem=recv_sem.at[block, kv],
            device_id={"ctx": to},
            device_id_type=pl.DeviceIdType.MESH,
        )

    own = (k_ref, v_ref)
    for kv in range(2):
        pl.when(not_top)(lambda: copy(me, kv, UP, up, own[kv]).start())
        pl.when(not_bottom)(lambda: copy(me, kv, DOWN, down, own[kv]).start())
        copy(me, kv, SIDE, side, own[kv]).start()
        copy(me, kv, TWIN, twin, own[kv]).start()

    def at(zz, yy, cc):
        return zz * lanes + yy * 2 + cc

    paired = jnp.minimum(z, zs - 1 - z)
    longer = jnp.where(z > zs - 1 - z, -1, 1)

    def level(r):
        near = jnp.where(lax.rem(r, 2) == 1, (r + 1) // 2, -((r + 1) // 2))
        return z + jnp.where(r <= 2 * paired, near, longer * (r - paired))

    def from_line(r):
        zz = level(r)
        block = at(zz, y, c)
        onward = jnp.where(zz < z, up, down)
        below = (zz < z).astype(jnp.int32)
        keep = below * not_top.astype(jnp.int32) + (1 - below) * not_bottom.astype(jnp.int32)
        for kv in range(2):
            copy(block, kv, UP, onward).wait_recv()
            pl.when(keep == 1)(lambda: copy(block, kv, UP, onward).start())
            copy(block, kv, SIDE, side).start()
            copy(block, kv, TWIN, twin).start()

    def from_side(r):
        block = at(level(r), 1 - y, c)
        for kv in range(2):
            copy(block, kv, TWIN, twin).wait_recv()
            copy(block, kv, TWIN, twin).start()

    factor = math.log2(math.e) / math.sqrt(head_size)
    first = order_ref[2 * me]
    second = order_ref[2 * me + 1]
    p = jnp.minimum(first, second)
    low_at = (second < first).astype(jnp.int32)
    ahead = lax.broadcasted_iota(jnp.int32, (span, span), 1) - lax.broadcasted_iota(
        jnp.int32, (span, span), 0
    )
    halves = (slice(0, span), slice(span, 2 * span))

    def facts(d):
        a = order_ref[2 * d]
        b = order_ref[2 * d + 1]
        return (b < a), jnp.minimum(a, b) < p

    def pick(flag, a, b):
        if isinstance(flag, bool):
            return a if flag else b
        return jnp.where(flag, a, b)

    def scores(q, keys):
        return (
            lax.dot_general(q, keys, (((1,), (1,)), ((), ())), preferred_element_type=jnp.float32)
            * factor
        )

    def wide(x):
        return jnp.concatenate([x, x], axis=1)

    def fill_first(slot, ks, vs, swapped):
        k1[halves[slot], :] = jnp.where(swapped, ks[1], ks[0])
        v1[halves[slot], :head_size] = jnp.where(swapped, vs[1], vs[0])

    def fill_second(slot, key, value, is_low):
        k2[halves[slot], :] = key
        zero = jnp.zeros_like(value)
        v2[halves[slot], :head_size] = pick(is_low, value, zero)
        v2[halves[slot], head_size:] = pick(is_low, zero, value)

    def pieces(d, is_own=False):
        if is_own:
            return [k_ref[s, :] for s in halves], [v_ref[s, :] for s in halves]
        return [buf[d, 0, s, :] for s in halves], [buf[d, 1, s, :] for s in halves]

    def high_update(h):
        score = scores(qs[1, h], k1[...])
        old = top[0, h]
        fresh = jnp.maximum(old, jnp.max(score, axis=1, keepdims=True))
        weight = jnp.exp2(score - wide(fresh)).astype(jnp.bfloat16)
        fade = jnp.exp2(old - fresh)
        add = jnp.dot(weight, v1[...], preferred_element_type=jnp.float32)
        acc[h] = acc[h] * wide(fade) + add
        top[0, h] = fresh

    def mixed_update(h, lows, diagonal=False):
        old_low, old_high = top[1, h], top[2, h]
        fresh_low, fresh_high = old_low, old_high
        made = []
        for j, is_low in enumerate(lows):
            score = scores(pick(is_low, qs[0, h], qs[1, h]), k2[halves[j], :])
            if diagonal:
                score = jnp.where(ahead <= 0, score, NEG)
            most = jnp.broadcast_to(jnp.max(score, axis=1, keepdims=True), score.shape)
            fresh_low = pick(is_low, jnp.maximum(fresh_low, most), fresh_low)
            fresh_high = pick(is_low, fresh_high, jnp.maximum(fresh_high, most))
            made.append(score)
        fade_low = jnp.exp2(old_low - fresh_low)
        fade_high = jnp.exp2(old_high - fresh_high)
        part_low = part[0, h] * fade_low
        part_high = part[1, h] * fade_high
        weights = []
        for score, is_low in zip(made, lows):
            weight = jnp.exp2(score - pick(is_low, fresh_low, fresh_high))
            part_low = pick(is_low, part_low + weight, part_low)
            part_high = pick(is_low, part_high, part_high + weight)
            weights.append(weight.astype(jnp.bfloat16))
        size = len(lows) * span
        add = jnp.dot(
            jnp.concatenate(weights, axis=1), v2[:size, :], preferred_element_type=jnp.float32
        )
        mix[h] = mix[h] * jnp.concatenate([fade_low, fade_high], axis=1) + add
        top[1, h] = fresh_low
        top[2, h] = fresh_high
        part[0, h] = part_low
        part[1, h] = part_high

    top[...] = jnp.full_like(top, NEG)
    part[...] = jnp.zeros_like(part)
    acc[...] = jnp.zeros_like(acc)
    mix[...] = jnp.zeros_like(mix)
    v1[:, head_size:] = jnp.ones_like(v1[:, head_size:])

    ks, vs = pieces(me, True)
    swapped = low_at == 1
    for h in range(heads):
        cols = slice(h * head_size, (h + 1) * head_size)
        rows = [q_ref[s, cols] for s in halves]
        qs[0, h] = jnp.where(swapped, rows[1], rows[0])
        qs[1, h] = jnp.where(swapped, rows[0], rows[1])
    fill_first(0, ks, vs, swapped)
    fill_second(0, jnp.where(swapped, ks[1], ks[0]), jnp.where(swapped, vs[1], vs[0]), True)
    fill_second(1, jnp.where(swapped, ks[0], ks[1]), jnp.where(swapped, vs[0], vs[1]), False)
    for h in range(heads):
        mixed_update(h, (True, False), diagonal=True)

    def fill_remote(d, slot1, slot2):
        ks, vs = pieces(d)
        swapped, is_low = facts(d)
        fill_first(slot1, ks, vs, swapped)
        other = jnp.logical_xor(swapped, jnp.logical_not(is_low))
        fill_second(
            slot2, jnp.where(other, ks[1], ks[0]), jnp.where(other, vs[1], vs[0]), is_low
        )
        return is_low

    def arrived(d):
        for kv in range(2):
            copy(d, kv, TWIN, twin).wait_recv()

    arrived(twin)
    is_low = fill_remote(twin, 1, 0)
    for h in range(heads):
        high_update(h)
        mixed_update(h, (is_low,))
    from_line(jnp.int32(1))

    last = 2 * zs - 2

    def step(t, carry):
        ends = (t == last).astype(jnp.int32)
        sideways = jnp.maximum(lax.rem(t, 2), ends)
        k = jnp.where(ends == 1, zs - 1, t // 2)

        @pl.when(sideways == 1)
        def _():
            from_side(k)

        @pl.when((1 - sideways) * (k + 2 < zs).astype(jnp.int32) == 1)
        def _():
            from_line(k + 2)

        zz = level(jnp.where(sideways == 1, k, k + 1))
        yy = jnp.where(sideways == 1, 1 - y, y)
        near = at(zz, yy, c)
        far = at(zz, yy, 1 - c)
        arrived(far)
        lows = (fill_remote(near, 0, 0), fill_remote(far, 1, 1))
        for h in range(heads):
            high_update(h)
            mixed_update(h, lows)
        return carry

    lax.fori_loop(0, last + 1, step, 0)

    for h in range(heads):
        cols = slice(h * head_size, (h + 1) * head_size)
        sum_low = jnp.sum(part[0, h], axis=1, keepdims=True)
        sum_high = jnp.sum(part[1, h], axis=1, keepdims=True)
        most = jnp.maximum(top[0, h], top[2, h])
        fade1 = jnp.exp2(top[0, h] - most)
        fade2 = jnp.exp2(top[2, h] - most)
        low = mix[h, :, :head_size] / sum_low
        high = (acc[h, :, :head_size] * fade1 + mix[h, :, head_size:] * fade2) / (
            acc[h, :, head_size:] * fade1 + sum_high * fade2
        )
        out_ref[halves[0], cols] = jnp.where(swapped, high, low).astype(jnp.bfloat16)
        out_ref[halves[1], cols] = jnp.where(swapped, low, high).astype(jnp.bfloat16)

    for kv in range(2):
        pl.when(not_top)(lambda: copy(me, kv, UP, up, own[kv]).wait_send())
        pl.when(not_bottom)(lambda: copy(me, kv, DOWN, down, own[kv]).wait_send())
        copy(me, kv, SIDE, side, own[kv]).wait_send()
        copy(me, kv, TWIN, twin, own[kv]).wait_send()

    def line_sent(r, carry):
        zz = level(r)
        block = at(zz, y, c)
        onward = jnp.where(zz < z, up, down)
        below = (zz < z).astype(jnp.int32)
        keep = below * not_top.astype(jnp.int32) + (1 - below) * not_bottom.astype(jnp.int32)
        for kv in range(2):
            pl.when(keep == 1)(lambda: copy(block, kv, UP, onward).wait_send())
            copy(block, kv, SIDE, side).wait_send()
            copy(block, kv, TWIN, twin).wait_send()
        return carry

    lax.fori_loop(1, zs, line_sent, 0)

    def side_sent(r, carry):
        for kv in range(2):
            copy(at(r, 1 - y, c), kv, TWIN, twin).wait_send()
        return carry

    lax.fori_loop(0, zs, side_sent, 0)


def body(n, queries, keys, values, span_order):
    local_rows, width = queries.shape
    head_size = keys.shape[1]
    heads = width // head_size
    span = local_rows // 2
    vmem = pl.BlockSpec(memory_space=pltpu.VMEM)
    return pl.pallas_call(
        functools.partial(attend_kernel, n, heads, span),
        out_shape=jax.ShapeDtypeStruct((local_rows, width), jnp.bfloat16),
        in_specs=[vmem, vmem, vmem, pl.BlockSpec(memory_space=pltpu.SMEM)],
        out_specs=vmem,
        scratch_shapes=[
            pltpu.VMEM((n, 2, local_rows, head_size), jnp.bfloat16),
            pltpu.VMEM((2, heads, span, head_size), jnp.bfloat16),
            pltpu.VMEM((local_rows, head_size), jnp.bfloat16),
            pltpu.VMEM((local_rows, 2 * head_size), jnp.bfloat16),
            pltpu.VMEM((local_rows, head_size), jnp.bfloat16),
            pltpu.VMEM((local_rows, 2 * head_size), jnp.bfloat16),
            pltpu.VMEM((3, heads, span, head_size), jnp.float32),
            pltpu.VMEM((2, heads, span, head_size), jnp.float32),
            pltpu.VMEM((heads, span, 2 * head_size), jnp.float32),
            pltpu.VMEM((heads, span, 2 * head_size), jnp.float32),
            pltpu.SemaphoreType.DMA((n, 2, 4)),
            pltpu.SemaphoreType.DMA((n, 2)),
        ],
        compiler_params=pltpu.CompilerParams(collective_id=0, has_side_effects=True),
        name="attend",
    )(queries, keys, values, span_order)


def solution(mesh):
    in_specs = (
        P(("groups", "ctx"), None),
        P(("groups", "ctx"), None),
        P(("groups", "ctx"), None),
        P("groups"),
    )
    out_specs = P(("groups", "ctx"), None)
    return jax.shard_map(
        functools.partial(body, mesh.shape["ctx"]),
        mesh=mesh,
        in_specs=in_specs,
        out_specs=out_specs,
        check_vma=False,
    )
```

```python
import functools
import math

import jax
import jax.numpy as jnp
from jax import lax
from jax.experimental import pallas as pl
from jax.experimental.pallas import tpu as pltpu
from jax.sharding import PartitionSpec as P

UP, DOWN, SIDE, TWIN = 0, 1, 2, 3
NEG = -1e30


def gather_kernel(n, k_ref, v_ref, buf, send_sem, recv_sem):
    lanes = 4
    zs = n // lanes
    me = lax.axis_index("ctx")
    z = me // lanes
    lane = lax.rem(me, lanes)
    y = lane // 2
    c = lax.rem(lane, 2)
    side = z * lanes + (1 - y) * 2 + c
    twin = z * lanes + y * 2 + (1 - c)
    not_top = z < zs - 1
    not_bottom = z > 0
    up = jnp.minimum(me + lanes, n - lanes + lane)
    down = jnp.maximum(me - lanes, lane)
    target = (up, down, side, twin)

    barrier = pltpu.get_barrier_semaphore()

    def greet(who):
        pl.semaphore_signal(
            barrier, inc=1, device_id={"ctx": who}, device_id_type=pl.DeviceIdType.MESH
        )

    greet(side)
    greet(twin)
    pl.when(not_top)(lambda: greet(up))
    pl.when(not_bottom)(lambda: greet(down))
    pl.semaphore_wait(barrier, 2 + not_top.astype(jnp.int32) + not_bottom.astype(jnp.int32))

    def copy(block, kv, route, src=None):
        return pltpu.make_async_remote_copy(
            src_ref=buf.at[block, kv] if src is None else src,
            dst_ref=buf.at[block, kv],
            send_sem=send_sem.at[block, kv, route],
            recv_sem=recv_sem.at[block, kv],
            device_id={"ctx": target[route]},
            device_id_type=pl.DeviceIdType.MESH,
        )

    own = (k_ref, v_ref)
    for kv in range(2):
        pl.when(not_top)(lambda: copy(me, kv, UP, own[kv]).start())
        pl.when(not_bottom)(lambda: copy(me, kv, DOWN, own[kv]).start())
        copy(me, kv, SIDE, own[kv]).start()
        copy(me, kv, TWIN, own[kv]).start()
    buf[me, 0] = k_ref[...]
    buf[me, 1] = v_ref[...]

    def at(zz, yy, cc):
        return zz * lanes + yy * 2 + cc

    def from_line(zz, onward, keep):
        block = at(zz, y, c)
        for kv in range(2):
            copy(block, kv, onward).wait_recv()
            pl.when(keep)(lambda: copy(block, kv, onward).start())
            copy(block, kv, SIDE).start()
            copy(block, kv, TWIN).start()

    def from_side(zz):
        block = at(zz, 1 - y, c)
        for kv in range(2):
            copy(block, kv, TWIN).wait_recv()
            copy(block, kv, TWIN).start()

    def from_twin(zz):
        for yy in (y, 1 - y):
            for kv in range(2):
                copy(at(zz, yy, 1 - c), kv, TWIN).wait_recv()

    def both(s, low, high):
        pl.when(z >= s)(lambda: low(z - s))
        pl.when(z + s < zs)(lambda: high(z + s))

    for s in range(1, zs):
        both(s, lambda zz: from_line(zz, UP, not_top), lambda zz: from_line(zz, DOWN, not_bottom))
        if s == 1:
            from_side(z)
        else:
            both(s - 1, from_side, from_side)
    both(zs - 1, from_side, from_side)
    from_twin(z)
    for s in range(1, zs):
        both(s, from_twin, from_twin)

    for kv in range(2):
        pl.when(not_top)(lambda: copy(me, kv, UP, own[kv]).wait_send())
        pl.when(not_bottom)(lambda: copy(me, kv, DOWN, own[kv]).wait_send())
        copy(me, kv, SIDE, own[kv]).wait_send()
        copy(me, kv, TWIN, own[kv]).wait_send()

    def line_sent(zz, onward, keep):
        for kv in range(2):
            pl.when(keep)(lambda: copy(at(zz, y, c), kv, onward).wait_send())
            copy(at(zz, y, c), kv, SIDE).wait_send()
            copy(at(zz, y, c), kv, TWIN).wait_send()

    def side_sent(zz):
        for kv in range(2):
            copy(at(zz, 1 - y, c), kv, TWIN).wait_send()

    side_sent(z)
    for s in range(1, zs):
        both(s, lambda zz: line_sent(zz, UP, not_top), lambda zz: line_sent(zz, DOWN, not_bottom))
        both(s, side_sent, side_sent)


def attend_kernel(
    n, heads, span, q_ref, kv_ref, order_ref, out_ref, qs, k1, v1, k2, v2, raw1, raw2, w1, w2
):
    head_size = k1.shape[1]
    me = lax.axis_index("ctx")
    first = order_ref[2 * me]
    second = order_ref[2 * me + 1]
    p = jnp.minimum(first, second)
    swapped = second < first
    low_at = swapped.astype(jnp.int32)
    pad_high = lax.rem(p, 2)
    pad_low = 1 - pad_high
    chunks_low = (p + 1 + pad_low) // 2
    halves = (slice(0, span), slice(span, 2 * span))

    def rows_of(slot):
        return pl.ds(pl.multiple_of(slot * span, span), span)

    def put(slot, block, half, is_low):
        k2[rows_of(slot), :] = kv_ref[block, 0, rows_of(half), :]
        value = kv_ref[block, 1, rows_of(half), :]
        zero = jnp.zeros_like(value)
        v2[rows_of(slot), :head_size] = jnp.where(is_low, value, zero)
        v2[rows_of(slot), head_size:] = jnp.where(is_low, zero, value)

    put(1, me, low_at, True)
    put(n, me, low_at, False)
    put(0, me, low_at, True)
    put(n + 1, me, 1 - low_at, False)

    def place(d, carry):
        q = jnp.minimum(order_ref[2 * d], order_ref[2 * d + 1])
        lo = (order_ref[2 * d + 1] < order_ref[2 * d]).astype(jnp.int32)
        is_low = q < p

        @pl.when(q != p)
        def _():
            slot = jnp.where(is_low, q + 1 + pad_low, n + 1 - pad_high - (q - p))
            put(slot, d, jnp.where(is_low, lo, 1 - lo), is_low)

        k1[rows_of(d), :] = kv_ref[d, 0, rows_of(lo), :]
        v1[rows_of(d), :head_size] = kv_ref[d, 1, rows_of(lo), :]
        return carry

    lax.fori_loop(0, n, place, 0)
    v1[:, head_size:] = jnp.ones_like(v1[:, head_size:])
    for h in range(heads):
        cols = slice(h * head_size, (h + 1) * head_size)
        pair = [q_ref[s, cols] for s in halves]
        qs[0, h] = jnp.where(swapped, pair[1], pair[0])
        qs[1, h] = jnp.where(swapped, pair[0], pair[1])

    factor = math.log2(math.e) / math.sqrt(head_size)
    ahead = lax.broadcasted_iota(jnp.int32, (span, span), 1) - lax.broadcasted_iota(
        jnp.int32, (span, span), 0
    )
    kept_first = jnp.concatenate([ahead <= 0, ahead <= span - 2 * span * pad_low], axis=1)
    kept_last = jnp.concatenate([ahead <= span - 2 * span * pad_high, ahead <= 0], axis=1)
    chunks1 = n // 2
    chunks2 = n // 2 + 1
    wide = 2 * span

    def scores(q, keys):
        return (
            lax.dot_general(q, keys, (((1,), (1,)), ((), ())), preferred_element_type=jnp.float32)
            * factor
        )

    def folded(x, op):
        return op(x[:, :span], x[:, span:])

    def one_head(h, b):
        high = jnp.full((span, span), NEG, jnp.float32)
        low = high
        for i in range(chunks1):
            cols = slice(i * wide, (i + 1) * wide)
            score = scores(qs[1, h], k1[cols, :])
            raw1[b, :, cols] = score
            high = jnp.maximum(high, folded(score, jnp.maximum))
        for i in range(chunks2):
            cols = slice(i * wide, (i + 1) * wide)
            is_low = i < chunks_low
            score = scores(qs[1 - is_low.astype(jnp.int32), h], k2[cols, :])
            if i == 0:
                score = jnp.where(kept_first, score, NEG)
            if i == chunks2 - 1:
                score = jnp.where(kept_last, score, NEG)
            raw2[b, :, cols] = score
            most = folded(score, jnp.maximum)
            low = jnp.where(is_low, jnp.maximum(low, most), low)
            high = jnp.where(is_low, high, jnp.maximum(high, most))
        low = jnp.broadcast_to(jnp.max(low, axis=1, keepdims=True), (span, span))
        high = jnp.broadcast_to(jnp.max(high, axis=1, keepdims=True), (span, span))
        for i in range(chunks1):
            cols = slice(i * wide, (i + 1) * wide)
            shift = jnp.concatenate([high, high], axis=1)
            w1[b, :, cols] = jnp.exp2(raw1[b, :, cols] - shift).astype(jnp.bfloat16)
        sum_low = jnp.zeros((span, span), jnp.float32)
        sum_high = sum_low
        for i in range(chunks2):
            cols = slice(i * wide, (i + 1) * wide)
            is_low = i < chunks_low
            shift = jnp.where(is_low, low, high)
            weight = jnp.exp2(raw2[b, :, cols] - jnp.concatenate([shift, shift], axis=1))
            w2[b, :, cols] = weight.astype(jnp.bfloat16)
            add = folded(weight, jnp.add)
            sum_low = jnp.where(is_low, sum_low + add, sum_low)
            sum_high = jnp.where(is_low, sum_high, sum_high + add)
        got1 = jnp.dot(w1[b], v1[...], preferred_element_type=jnp.float32)
        got2 = jnp.dot(w2[b], v2[...], preferred_element_type=jnp.float32)
        sum_low = jnp.sum(sum_low, axis=1, keepdims=True)
        sum_high = jnp.sum(sum_high, axis=1, keepdims=True)
        out_low = got2[:, :head_size] / sum_low
        out_high = (got1[:, :head_size] + got2[:, head_size:]) / (got1[:, head_size:] + sum_high)
        cols = pl.ds(pl.multiple_of(h * head_size, head_size), head_size)
        out_ref[halves[0], cols] = jnp.where(swapped, out_high, out_low).astype(jnp.bfloat16)
        out_ref[halves[1], cols] = jnp.where(swapped, out_low, out_high).astype(jnp.bfloat16)

    together = 2 if chunks1 <= heads else 1

    def some_heads(g, carry):
        for b in range(together):
            one_head(g * together + b, b)
        return carry

    lax.fori_loop(0, heads // together, some_heads, 0)


def body(n, queries, keys, values, span_order):
    local_rows, width = queries.shape
    head_size = keys.shape[1]
    heads = width // head_size
    span = local_rows // 2
    vmem = pl.BlockSpec(memory_space=pltpu.VMEM)
    gathered = pl.pallas_call(
        functools.partial(gather_kernel, n),
        out_shape=jax.ShapeDtypeStruct((n, 2, local_rows, head_size), jnp.bfloat16),
        in_specs=[vmem, vmem],
        out_specs=vmem,
        scratch_shapes=[
            pltpu.SemaphoreType.DMA((n, 2, 4)),
            pltpu.SemaphoreType.DMA((n, 2)),
        ],
        compiler_params=pltpu.CompilerParams(collective_id=0, has_side_effects=True),
        name="gather",
    )(keys, values)
    half_keys = n * span
    more_keys = (n + 2) * span
    return pl.pallas_call(
        functools.partial(attend_kernel, n, heads, span),
        out_shape=jax.ShapeDtypeStruct((local_rows, width), jnp.bfloat16),
        in_specs=[vmem, vmem, pl.BlockSpec(memory_space=pltpu.SMEM)],
        out_specs=vmem,
        scratch_shapes=[
            pltpu.VMEM((2, heads, span, head_size), jnp.bfloat16),
            pltpu.VMEM((half_keys, head_size), jnp.bfloat16),
            pltpu.VMEM((half_keys, 2 * head_size), jnp.bfloat16),
            pltpu.VMEM((more_keys, head_size), jnp.bfloat16),
            pltpu.VMEM((more_keys, 2 * head_size), jnp.bfloat16),
            pltpu.VMEM((2, span, half_keys), jnp.float32),
            pltpu.VMEM((2, span, more_keys), jnp.float32),
            pltpu.VMEM((2, span, half_keys), jnp.bfloat16),
            pltpu.VMEM((2, span, more_keys), jnp.bfloat16),
        ],
        name="attend",
    )(queries, gathered, span_order)


def solution(mesh):
    in_specs = (
        P(("groups", "ctx"), None),
        P(("groups", "ctx"), None),
        P(("groups", "ctx"), None),
        P("groups"),
    )
    out_specs = P(("groups", "ctx"), None)
    return jax.shard_map(
        functools.partial(body, mesh.shape["ctx"]),
        mesh=mesh,
        in_specs=in_specs,
        out_specs=out_specs,
        check_vma=False,
    )
```
